32 devices in a mesh: seq: 4 (over x, core), chan: 4 (over z), batch: 2 (over y).
Axes of the slice: x: 2, y: 2, z: 4, core: 2. Of those that a mesh axis runs over, the one named last changes fastest.
Arguments:
- tokens: bfloat16 [2048, 4096], P(('batch', 'seq'), 'chan'), parts along dimension 0, may hold values from -6 to 6
- in_weights: bfloat16 [3, 4096, 4096], P(None, 'seq', 'chan'), may hold values from -0.09375 to 0.09375
- out_weights: bfloat16 [4096, 4096], P('seq', 'chan'), may hold values from -0.09375 to 0.09375
- spectrum: float32 [2, 4096, 2048], P(None, 'chan', 'seq'), may hold values from -6 to 6
Outputs:
- output: bfloat16 [2048, 4096], P(('batch', 'seq'), 'chan'), parts along dimension 0
The draws below stay inside these ranges and needn't reach their ends.
There are 2 independent parts, one for each index of `batch`. The reference program is written for one: setup_inputs(seed, part) draws one part's arguments, and reference() takes and returns one part's arrays. A program takes and returns all parts, laid end to end along the dimension named above; an argument that names none is the same for every part. Nothing has to cross between parts.
All inputs are finite; a program needn't handle non-finite values.
Results may differ from the reference program's by a relative error of at most 0.014.
Values may be sent and summed in bfloat16 or wider, within the bound.
No kernel may reach another device: no remote copies, remote signals or barrier semaphores. Data moves between devices by JAX's collectives and lax.ppermute only.
A program may use at most 128 MiB of HBM per device.

```python
import jax
import jax.numpy as jnp

D = 4096
LENGTH = 1024
FFT_LEN = 2048


def levels(key, extent, cuts, smallest, largest):
    gain = 1.0
    for axis_at, parts in cuts:
        draws = jax.random.uniform(jax.random.fold_in(jax.random.fold_in(key, 6), axis_at), (parts,), jnp.float32, smallest / len(cuts), largest / len(cuts))
        gain = gain * jnp.repeat(jnp.exp(draws), extent[axis_at] // parts).reshape((-1,) + (1,) * (len(extent) - 1 - axis_at))
    return gain


def centred(stream_key, shape, width, limit, split=(), kind=jnp.bfloat16):
    array = jax.random.normal(stream_key, shape, jnp.float32) * width
    if len(split) > 0:
        array = levels(stream_key, shape, split, -0.22, 0.18) * array
    return jnp.clip(array, min=-limit, max=limit).astype(kind)


def setup_inputs(seed: int = 0, part: int = 0) -> dict:
    splits = jax.random.split(jax.random.key(seed), 5)
    part_keys = jax.random.split(jax.random.fold_in(splits[4], part), 5)
    return {
        "tokens": centred(part_keys[0], (LENGTH, D), 1.0, 6.0, ((0, 4), (1, 4))),
        "in_weights": centred(splits[1], (3, D, D), D ** -0.5, 0.09375, ((1, 4), (2, 4))),
        "out_weights": centred(splits[2], (D, D), D ** -0.5, 0.09375, ((0, 4), (1, 4))),
        "spectrum": centred(splits[3], (2, D, FFT_LEN), 1.0, 6.0, ((1, 4), (2, 4)), jnp.float32),
    }


def reference(tokens, in_weights, out_weights, spectrum):
    outer_gate = jnp.dot(tokens, in_weights[0], preferred_element_type=jnp.float32)
    inner_gate = jnp.dot(tokens, in_weights[1], preferred_element_type=jnp.float32)
    value_proj = jnp.dot(tokens, in_weights[2], preferred_element_type=jnp.float32)
    gated = inner_gate * value_proj
    padded = jnp.concatenate([gated, jnp.zeros_like(gated)], axis=0)
    spectra_in = jnp.fft.fft(padded, axis=0)
    filters = jnp.transpose(spectrum[0]) + 1j * jnp.transpose(spectrum[1])
    convolved = jnp.real(jnp.fft.ifft(spectra_in * filters, axis=0))[:LENGTH]
    convolved = convolved.astype(jnp.float32)
    mixed = (outer_gate * convolved).astype(jnp.bfloat16)
    return jnp.dot(mixed, out_weights, preferred_element_type=jnp.float32).astype(jnp.bfloat16)
```

```python
import math

import jax
import jax.numpy as jnp
from jax import lax
from jax.sharding import PartitionSpec as P

bf16 = jnp.bfloat16
f32 = jnp.float32

TABLE_BYTES = 2**24


def after(value, *earlier):
    return lax.optimization_barrier((value, *earlier))[0]


def turn_parts(rows, columns, period):
    angle = ((rows[:, None] * columns[None, :]) % period).astype(f32) * (2.0 * math.pi / period)
    return jnp.cos(angle), jnp.sin(angle)


def turn_table(rows_hi, rows_lo, columns, period):
    hi_cos, hi_sin, lo_cos, lo_sin = lax.optimization_barrier(
        turn_parts(rows_hi, columns, period) + turn_parts(rows_lo, columns, period)
    )
    cos = hi_cos[:, None] * lo_cos[None] - hi_sin[:, None] * lo_sin[None]
    sin = hi_sin[:, None] * lo_cos[None] + hi_cos[:, None] * lo_sin[None]
    shape = (rows_hi.shape[0] * rows_lo.shape[0], columns.shape[0])
    return cos.astype(bf16).reshape(shape), sin.astype(bf16).reshape(shape)


def body(tokens, in_weights, out_weights, spectrum):
    seq = lax.axis_size("seq")
    chan = lax.axis_size("chan")
    batch = lax.axis_size("batch")
    me_seq, me_chan, me_batch = (lax.axis_index(a) for a in ("seq", "chan", "batch"))
    tok_rows, features = tokens.shape
    length = seq * tok_rows
    period = 2 * length
    sub = in_weights.shape[2] // seq
    freqs = spectrum.shape[2]

    def flip(value, bits):
        return lax.ppermute(value, "seq", [(i, i ^ bits) for i in range(seq)])

    def ring(value):
        return lax.ppermute(value, "chan", [(i, (i + 1) % chan) for i in range(chan)])

    def other_batch(value):
        return lax.ppermute(value, "batch", [(0, 1), (1, 0)])

    def far_flip(value, bits, axis):
        if batch != 2:
            return flip(value, bits)
        half = value.shape[axis] // 2
        mine = flip(lax.dynamic_slice_in_dim(value, me_batch * half, half, axis), bits)
        theirs = other_batch(mine)
        first = jnp.where(me_batch == 0, mine, theirs)
        second = jnp.where(me_batch == 0, theirs, mine)
        return jnp.concatenate([first, second], axis)

    def sub_channels(value, bits, axis):
        return lax.dynamic_slice_in_dim(value, (me_seq ^ bits) * sub, sub, axis)

    evens, odds = list(range(0, seq, 2)), list(range(1, seq, 2))
    order = evens + odds

    near = tokens
    far = [flip(tokens, bits) for bits in evens[1:]]
    far = jnp.concatenate(far, 0) if len(far) > 1 else far[0]
    gathered = []
    for step in range(chan):
        if step > 0:
            near, far = ring(near), ring(far)
        gathered.append(jnp.concatenate([near, far, flip(near, 1), flip(far, 1)], 0))

    w_parts = []
    for bits in range(seq):
        part = sub_channels(in_weights, bits, 2)
        if bits == 1:
            part = flip(part, 1)
        elif bits > 1:
            part = far_flip(part, bits, 1)
        w_parts.append(part)
    w_rows = jnp.stack(w_parts)

    narrow = spectrum.astype(bf16)
    filters = []
    for bits in range(seq):
        part = sub_channels(narrow, bits, 1)
        if bits == 1:
            part = flip(part, 1)
        elif bits > 1:
            part = far_flip(part, bits, 1)
        filters.append(part)

    out_parts = {0: out_weights, 1: flip(out_weights, 1)}
    for bits in evens[1:]:
        out_parts[bits] = far_flip(out_weights, bits, 0)
        out_parts[bits + 1] = flip(out_parts[bits], 1)
    out_rows = jnp.stack([out_parts[bits] for bits in range(seq)])

    projected = 0.0
    for step in range(chan):
        block = (me_chan - step) % chan
        w_block = lax.dynamic_index_in_dim(w_rows, me_seq ^ block, 0, keepdims=False)
        projected = projected + jnp.einsum(
            "nk,pkc->pnc", gathered[step], w_block, preferred_element_type=f32
        )
    outer_gate = projected[0]
    gated = (projected[1] * projected[2]).astype(bf16)

    low = math.gcd(tok_rows, 32)
    starts = jnp.stack([(me_seq ^ bits) * tok_rows for bits in order])
    rows_hi = (starts[:, None] + low * jnp.arange(tok_rows // low)[None]).reshape(-1)
    rows_lo = jnp.arange(low)
    convolved = 0.0
    for bits in range(seq):
        columns = (me_seq ^ bits) * freqs + jnp.arange(freqs)
        if bits > 0 and 4 * length * period > TABLE_BYTES:
            columns = after(columns, convolved)
        cos, sin = turn_table(rows_hi, rows_lo, columns, period)
        g_real = jnp.einsum("nc,nk->ck", gated, cos, preferred_element_type=f32)
        g_imag = jnp.einsum("nc,nk->ck", gated, sin, preferred_element_type=f32)
        h_real, h_imag = filters[bits][0].astype(f32), filters[bits][1].astype(f32)
        y_real = (g_real * h_real + g_imag * h_imag).astype(bf16)
        y_imag = (g_real * h_imag - g_imag * h_real).astype(bf16)
        convolved = convolved + jnp.einsum("nk,ck->nc", cos, y_real, preferred_element_type=f32)
        convolved = convolved - jnp.einsum("nk,ck->nc", sin, y_imag, preferred_element_type=f32)
    mixed = (outer_gate * (convolved * (1.0 / period))).astype(bf16)

    own = jnp.zeros((tok_rows, seq * sub), bf16)
    for place, bits in enumerate(order):
        part = mixed[place * tok_rows : (place + 1) * tok_rows]
        if bits > 0:
            part = flip(part, bits)
        own = lax.dynamic_update_slice_in_dim(own, part, (me_seq ^ bits) * sub, 1)
    result = 0.0
    for step in range(chan):
        if step > 0:
            own = ring(own)
        block = (me_chan - step) % chan
        w_block = lax.dynamic_index_in_dim(out_rows, me_seq ^ block, 0, keepdims=False)
        result = result + jnp.dot(own, w_block, preferred_element_type=f32)
    return result.astype(bf16)


def solution(mesh):
    placed = (
        P(("batch", "seq"), "chan"),
        P(None, "seq", "chan"),
        P("seq", "chan"),
        P(None, "chan", "seq"),
    )
    return jax.shard_map(
        body, mesh=mesh, in_specs=placed, out_specs=P(("batch", "seq"), "chan"), check_vma=False
    )
```
